32 devices in a mesh: gx: 8 (over y, x, core), gy: 4 (over z).
Axes of the slice: x: 2, y: 2, z: 4, core: 2. Of those that a mesh axis runs over, the one named last changes fastest.
Arguments:
- features: bfloat16 [16384, 128], P(('gx', 'gy')), may hold values from -6 to 6
- cache_in: bfloat16 [16384, 128], replicated, may hold values from -26 to 26
- cache_hidden: bfloat16 [16384, 128], replicated, may hold values from -26 to 26
- tiles: bfloat16 [32, 32, 256, 256], P(('gx', 'gy')), may hold values from -0.0625 to 0.0625
- tile_pos: int32 [32, 32, 2], P(('gx', 'gy')), may hold values from 0 to 1
- order: int32 [2, 32], replicated, may hold values from 0 to 31, each once within a row
- skip: int32 [2, 32], replicated, may hold values 0 or 1
- w_first: bfloat16 [128, 128], replicated, may hold values from -0.5 to 0.5
- w_second: bfloat16 [128, 128], replicated, may hold values from -0.5 to 0.5
Outputs:
- output: bfloat16 [16384, 128], P(('gx', 'gy'))
- drift: float32 [2], replicated
The draws below stay inside these ranges and needn't reach their ends.
Inputs may be any that keep to these rules, and one draw needn't show every extreme that they name: `order`: each row names every block once.
All inputs are finite; a program needn't handle non-finite values.
Results may differ from the reference program's by a relative error of at most 0.0052.
Values may be sent and summed in bfloat16 or wider, within the bound.
A program may use at most 192 MiB of HBM per device.

```python
import jax
import jax.numpy as jnp
from jax import lax

F = 128
HID = 128
V_DEV = 512
NB = 32
TS = 256
V = 16384


def scaled_rows(key, width):
    total_rows = NB * V_DEV
    position = jnp.arange(total_rows, dtype=jnp.float32) / max(total_rows - 1, 1)
    noise = jnp.clip(jax.random.normal(key, (total_rows, width), jnp.float32), -6.0, 6.0)
    row_scale = 0.5 + 1.5 * position
    values = row_scale[:, None] * noise
    return values.astype(jnp.bfloat16)


def draw_cache_in(key, part):
    return scaled_rows(jax.random.fold_in(key, 11), F)


def draw_cache_hidden(key, part):
    return scaled_rows(jax.random.fold_in(key, 23), HID)


def plant(entries, key, least, high):
    place = [jax.random.randint(jax.random.fold_in(key, axis), (), 0, length) for axis, length in enumerate(entries.shape)]
    main_axis = entries.shape.index(max(entries.shape))
    next_to = place[:main_axis] + [(place[main_axis] + 1) % entries.shape[main_axis]] + place[main_axis + 1:]
    return entries.at[tuple(place)].set(least).at[tuple(next_to)].set(high)


def levels(stream_key, shape, cuts, least, high):
    def one(dim, shards_of):
        draws = jax.random.uniform(jax.random.fold_in(jax.random.fold_in(stream_key, 6), dim), (shards_of,), jnp.float32, least / len(cuts), high / len(cuts))
        return jnp.repeat(jnp.exp(draws), shape[dim] // shards_of).reshape((-1,) + (1,) * (len(shape) - dim - 1))

    loudness = one(*cuts[0])
    for cut in cuts[1:]:
        loudness = loudness * one(*cut)
    return loudness


def bell_draw(stream_key, extent, scale, most, pieces=(), kind=jnp.bfloat16):
    entries = scale * jax.random.normal(stream_key, extent, jnp.float32)
    if pieces:
        entries = entries * levels(stream_key, extent, pieces, -0.22, 0.18)
    return jnp.clip(entries, -most, most).astype(kind)


def setup_inputs(seed: int = 0) -> dict:
    seeds = jax.random.split(jax.random.key(seed), 10)
    features = bell_draw(seeds[0], (V, F), 1.0, 6.0, ((0, 32),))
    cache_in = draw_cache_in(jax.random.fold_in(seeds[9], 71), 0)
    cache_hidden = draw_cache_hidden(jax.random.fold_in(seeds[9], 71), 0)
    tiles = bell_draw(seeds[3], (NB, NB, TS, TS), (NB * TS) ** -0.5, 0.0625, ((0, 32),))
    tile_pos = plant(jax.random.randint(seeds[4], (NB, NB, 2), 0, 2), jax.random.fold_in(seeds[4], 1), 0, 1).astype(jnp.int32)
    order = jax.vmap(lambda own: jax.random.permutation(own, NB))(jax.random.split(seeds[5], 2)).reshape((2, NB)).astype(jnp.int32)
    skip = plant((jax.random.randint(seeds[6], (2, NB), 0, 2) < 1).astype(jnp.int32), jax.random.fold_in(seeds[6], 1), 0, 1)
    w_first = bell_draw(seeds[7], (F, HID), F ** -0.5, 0.5)
    w_second = bell_draw(seeds[8], (HID, HID), HID ** -0.5, 0.5)
    return {"features": features, "cache_in": cache_in, "cache_hidden": cache_hidden, "tiles": tiles, "tile_pos": tile_pos, "order": order, "skip": skip, "w_first": w_first, "w_second": w_second}


def refreshed_flags(order, skip):
    round_hits = (order[:, :, None] == jnp.arange(NB, dtype=jnp.int32)[None, None, :]).astype(jnp.int32)
    return jnp.sum(round_hits * (1 - skip)[:, :, None], axis=1).astype(jnp.int32)


def aggregate(embed, cached, fresh_flags, tiles, tile_pos):
    feat_width = embed.shape[1]
    new_blocks = embed.reshape(NB, 2, TS, feat_width)
    old_blocks = cached.reshape(NB, 2, TS, feat_width)
    block_ids = jnp.arange(NB, dtype=jnp.int32)

    def per_block(operands):
        block_index, tile_row, pos_row = operands
        use_new = (fresh_flags == 1) | (block_ids == block_index)
        source = jnp.where(use_new[:, None, None, None], new_blocks, old_blocks)
        halves = jnp.where((pos_row[:, 1] == 0)[:, None, None], source[:, 0], source[:, 1])
        products = jnp.einsum("kab,kbf->kaf", tile_row.astype(jnp.float32), halves.astype(jnp.float32))
        upper = (pos_row[:, 0] == 0)[:, None, None]
        upper_sum = jnp.sum(jnp.where(upper, products, jnp.float32(0.0)), axis=0)
        lower_sum = jnp.sum(jnp.where(upper, jnp.float32(0.0), products), axis=0)
        return jnp.concatenate([upper_sum, lower_sum], axis=0)

    summed = lax.map(per_block, (block_ids, tiles, tile_pos))
    return summed.reshape(NB * V_DEV, feat_width)


def reference(features, cache_in, cache_hidden, tiles, tile_pos, order, skip, w_first, w_second):
    fresh_flags = refreshed_flags(order, skip)
    first_agg = aggregate(features, cache_in, fresh_flags[0], tiles, tile_pos).astype(jnp.bfloat16)
    hidden = jnp.maximum(jnp.dot(first_agg, w_first, preferred_element_type=jnp.float32), 0.0).astype(jnp.bfloat16)
    second_agg = aggregate(hidden, cache_hidden, fresh_flags[1], tiles, tile_pos).astype(jnp.bfloat16)
    output = jnp.dot(second_agg, w_second, preferred_element_type=jnp.float32).astype(jnp.bfloat16)
    input_change = features.astype(jnp.float32) - cache_in.astype(jnp.float32)
    hidden_change = hidden.astype(jnp.float32) - cache_hidden.astype(jnp.float32)
    drift = jnp.stack([jnp.sum(input_change * input_change) / (NB * V_DEV * F),
                       jnp.sum(hidden_change * hidden_change) / (NB * V_DEV * HID)])
    return output, drift
```

```python
import functools

import jax
import jax.numpy as jnp
from jax import lax
from jax.experimental import pallas as pl
from jax.experimental.pallas import tpu as pltpu
from jax.sharding import PartitionSpec as P

GROUP = 4
CACHE_SLOTS = 16
MESH = pl.DeviceIdType.MESH


def flip(value, bits):
    bit = 1
    while bit <= bits:
        if bits & bit:
            value = value + bit - 2 * bit * ((value // bit) % 2)
        bit *= 2
    return value


def hop_bit(d, k):
    low = d & -d
    high = 1 << (d.bit_length() - 1)
    return low if k % 2 == 0 else high


def pick(i, values):
    chosen = values[0]
    for t in range(1, len(values)):
        chosen = jnp.where(i == t, values[t], chosen)
    return chosen


def arrival_order(planes, depth):
    slots = [(d, k) for d in range(planes) for k in range(depth)]
    return sorted(slots, key=lambda s: (bin(s[0]).count("1") + s[1], s[1], s[0]))


def kernel(planes, depth, code_ref, feat_ref, cache_a, cache_b, tiles_ref, w1_ref, w2_ref,
           out_ref, drift_ref, got_a, got_b, tiles_v, cached, acc, parts,
           send_sems, recv_sems, cache_sems, tile_sem, feat_sem):
    half = planes * depth
    blocks = 2 * half
    rows = feat_ref.shape[0]
    tile_rows = rows // 2
    width = feat_ref.shape[1]
    gx = lax.axis_index("gx")
    gz = lax.axis_index("gy")
    plane = gx // 2
    core = gx % 2

    def device(c, d, k):
        return (flip(plane, d) * 2 + flip(core, c), flip(gz, k))

    def block_of(slot):
        x, z = device(*slot)
        return x * depth + z

    def slot_id(c, d, k):
        return c * half + d * depth + k

    got = (got_a, got_b)
    caches = (cache_a, cache_b)

    feat_copy = pltpu.make_async_copy(feat_ref, got_a.at[0], feat_sem)
    feat_copy.start()

    peers = [(1, 0, 0)] + [(0, 0, k) for k in range(1, depth)]
    bit = 1
    while bit < planes:
        peers.append((0, bit, 0))
        bit *= 2
    barrier = pltpu.get_barrier_semaphore()
    for peer in peers:
        pl.semaphore_signal(barrier, inc=1, device_id=device(*peer), device_id_type=MESH)
    pl.semaphore_wait(barrier, len(peers))

    def remote(layer, src, dst, hop):
        return pltpu.make_async_remote_copy(
            src_ref=got[layer].at[slot_id(*src)],
            dst_ref=got[layer].at[slot_id(*dst)],
            send_sem=send_sems.at[layer, slot_id(*dst)],
            recv_sem=recv_sems.at[layer, slot_id(*dst)],
            device_id=device(*hop),
            device_id_type=MESH,
        )

    def forwards(layer, d, k):
        copies = []
        bit = 1
        while bit < planes:
            if not d & bit and hop_bit(d | bit, k) == bit:
                copies.append(remote(layer, (0, d, k), (0, d | bit, k), (0, bit, 0)))
            bit *= 2
        if d == 0 and k == 0:
            for far in range(1, depth):
                copies.append(remote(layer, (0, 0, 0), (0, 0, far), (0, 0, far)))
        copies.append(remote(layer, (0, d, k), (1, d, k), (1, 0, 0)))
        return copies

    def wait_slot(layer, slot):
        remote(layer, slot, slot, (1, 0, 0)).wait_recv()

    order = arrival_order(planes, depth)
    groups = [order[i:i + GROUP] for i in range(0, half, GROUP)]
    folds = []
    for g, group in enumerate(groups):
        fold = [(0, d, k) for d, k in group]
        if g:
            fold = [(1, d, k) for d, k in groups[g - 1]] + fold
        folds.append(fold)
    folds.append([(1, d, k) for d, k in groups[-1]])
    uses = [(layer, slot) for layer in range(2) for fold in folds for slot in fold]

    def cache_copy(u):
        layer, slot = uses[u]
        start = pl.multiple_of(block_of(slot) * rows, rows)
        return pltpu.make_async_copy(
            caches[layer].at[pl.ds(start, rows)],
            cached.at[u % CACHE_SLOTS],
            cache_sems.at[u % CACHE_SLOTS],
        )

    def fold_slots(layer, fold, first_use):
        slot_values = [jnp.int32(slot_id(*s)) for s in fold]
        block_values = [block_of(s) for s in fold]

        def body(i, carry):
            s = pick(i, slot_values)
            j = pick(i, block_values)
            code = code_ref[layer, j]
            new = got[layer][s]
            old = cached[(first_use + i) % CACHE_SLOTS]
            change = new.astype(jnp.float32) - old.astype(jnp.float32)
            change = change * change
            parts[layer, j] = jnp.sum(change.reshape(rows // 8, 8, width), axis=0)
            source = lax.select(code >= 4, new, old)
            chosen = lax.select((code // 2) % 2 == 0, source[:tile_rows], source[tile_rows:])
            zeros = jnp.zeros_like(chosen)
            upper = code % 2 == 0
            spread = jnp.concatenate(
                [lax.select(upper, chosen, zeros), lax.select(upper, zeros, chosen)], axis=1
            )
            acc[...] += jnp.dot(tiles_v[j], spread, preferred_element_type=jnp.float32)
            return carry

        lax.fori_loop(0, len(fold), body, 0)

    use = 0
    tile_copy = pltpu.make_async_copy(tiles_ref.at[0], tiles_v, tile_sem)
    sent = []
    for layer in range(2):
        weight = (w1_ref, w2_ref)[layer]
        if layer == 0:
            feat_copy.wait()
        for g, fold in enumerate(folds):
            if g < len(groups):
                for d, k in groups[g]:
                    if (d, k) != (0, 0):
                        wait_slot(layer, (0, d, k))
                    for copy in forwards(layer, d, k):
                        copy.start()
                        sent.append(copy)
                    if layer == 0 and (d, k) == (0, 0):
                        tile_copy.start()
                        for u in range(min(CACHE_SLOTS, len(uses))):
                            cache_copy(u).start()
                        acc[...] = jnp.zeros_like(acc)
            if layer == 0 and g == 0:
                tile_copy.wait()
            for t, slot in enumerate(fold):
                if slot[0] == 1:
                    wait_slot(layer, slot)
                cache_copy(use + t).wait()
            fold_slots(layer, fold, use)
            for t in range(len(fold)):
                if use + t + CACHE_SLOTS < len(uses):
                    cache_copy(use + t + CACHE_SLOTS).start()
            use += len(fold)
        for part in range(2):
            agg = acc[:, part * width:(part + 1) * width].astype(jnp.bfloat16)
            mixed = jnp.dot(agg, weight[...], preferred_element_type=jnp.float32)
            place = pl.ds(part * tile_rows, tile_rows)
            if layer == 0:
                got_b[0, place] = jnp.maximum(mixed, 0.0).astype(jnp.bfloat16)
            else:
                out_ref[place] = mixed.astype(jnp.bfloat16)
        if layer == 0:
            acc[...] = jnp.zeros_like(acc)
    for layer in range(2):
        total = jnp.sum(jnp.sum(parts[layer], axis=0))
        drift_ref[layer] = total / (blocks * rows * width)
    for copy in sent:
        copy.wait_send()


def on_device(planes, depth, features, cache_in, cache_hidden, tiles, tile_pos, order, skip, w_first, w_second):
    own_index = lax.axis_index(("gx", "gy"))
    block_count = order.shape[1]
    rows, width = features.shape
    tile_rows = tiles.shape[2]
    ids = jnp.arange(block_count, dtype=jnp.int32)
    hits = order[:, :, None] == ids[None, None, :]
    fresh = jnp.sum(jnp.where(hits, (1 - skip)[:, :, None], 0), axis=1)
    fresh = jnp.where(ids[None, :] == own_index, 1, fresh)
    code = fresh * 4 + (tile_pos[0, :, 1] * 2 + tile_pos[0, :, 0])[None, :]
    vmem = pl.BlockSpec(memory_space=pltpu.VMEM)
    smem = pl.BlockSpec(memory_space=pltpu.SMEM)
    anywhere = pl.BlockSpec(memory_space=pl.ANY)
    return pl.pallas_call(
        functools.partial(kernel, planes, depth),
        out_shape=(
            jax.ShapeDtypeStruct((rows, width), jnp.bfloat16),
            jax.ShapeDtypeStruct((2,), jnp.float32),
        ),
        in_specs=[smem, anywhere, anywhere, anywhere, anywhere, vmem, vmem],
        out_specs=(vmem, smem),
        scratch_shapes=[
            pltpu.VMEM((block_count, rows, width), jnp.bfloat16),
            pltpu.VMEM((block_count, rows, width), jnp.bfloat16),
            pltpu.VMEM((block_count, tile_rows, tile_rows), jnp.bfloat16),
            pltpu.VMEM((CACHE_SLOTS, rows, width), jnp.bfloat16),
            pltpu.VMEM((tile_rows, 2 * width), jnp.float32),
            pltpu.VMEM((2, block_count, 8, width), jnp.float32),
            pltpu.SemaphoreType.DMA((2, block_count)),
            pltpu.SemaphoreType.DMA((2, block_count)),
            pltpu.SemaphoreType.DMA((CACHE_SLOTS,)),
            pltpu.SemaphoreType.DMA,
            pltpu.SemaphoreType.DMA,
        ],
        compiler_params=pltpu.CompilerParams(
            collective_id=0, has_side_effects=True, vmem_limit_bytes=60 * 1024 * 1024
        ),
    )(code, features, cache_in, cache_hidden, tiles, w_first, w_second)


def solution(mesh):
    in_specs = (
        P(("gx", "gy"), None),
        P(),
        P(),
        P(("gx", "gy"), None, None, None),
        P(("gx", "gy"), None, None),
        P(),
        P(),
        P(),
        P(),
    )
    out_specs = (P(("gx", "gy"), None), P())
    body = functools.partial(on_device, mesh.shape["gx"] // 2, mesh.shape["gy"])
    return jax.shard_map(body, mesh=mesh, in_specs=in_specs, out_specs=out_specs, check_vma=False)
```

```python
import functools

import jax
import jax.numpy as jnp
from jax import lax
from jax.experimental import pallas as pl
from jax.experimental.pallas import tpu as pltpu
from jax.sharding import PartitionSpec as P

GROUP = 4
CACHE_SLOTS = 16
CHUNKS = 2
COLUMN_COST = 2
PLANE_COST = 3
CHUNK_COST = 1
COLUMN_SHARE = 2
MESH = pl.DeviceIdType.MESH


def flip(value, bits):
    bit = 1
    while bit <= bits:
        if bits & bit:
            value = value + bit - 2 * bit * ((value // bit) % 2)
        bit *= 2
    return value


def hop_bit(d, part):
    low = d & -d
    high = 1 << (d.bit_length() - 1)
    return low if part % 2 == 0 else high


def by_column(d, k, part):
    return d & (d - 1) != 0 and 0 < k * CHUNKS + part < COLUMN_SHARE + CHUNKS and k > 0


def pick(i, values):
    chosen = values[0]
    for t in range(1, len(values)):
        chosen = jnp.where(i == t, values[t], chosen)
    return chosen


def arrival_order(planes, depth):
    events = [(d, k, h) for d in range(planes) for k in range(depth) for h in range(CHUNKS)]

    def expected(event):
        d, k, h = event
        return (COLUMN_COST * k + PLANE_COST * bin(d).count("1") + CHUNK_COST * h, k, d, h)

    return sorted(events, key=expected)


def kernel(planes, depth, code_ref, feat_ref, cache_a, cache_b, tiles_ref, w1_ref, w2_ref,
           out_ref, drift_ref, got_a, got_b, tiles_v, cached, acc, parts,
           send_sems, recv_sems, cache_sems, tile_sem, feat_sem):
    half = planes * depth
    blocks = 2 * half
    rows = feat_ref.shape[0]
    tile_rows = rows // 2
    width = feat_ref.shape[1]
    gx = lax.axis_index("gx")
    gz = lax.axis_index("gy")
    plane = gx // 2
    core = gx % 2

    def device(c, d, k):
        return (flip(plane, d) * 2 + flip(core, c), flip(gz, k))

    def block_of(slot):
        x, z = device(*slot)
        return x * depth + z

    def slot_id(c, d, k):
        return c * half + d * depth + k

    got = (got_a, got_b)
    caches = (cache_a, cache_b)

    feat_copy = pltpu.make_async_copy(feat_ref, got_a.at[0], feat_sem)
    feat_copy.start()

    peers = [(1, 0, 0)] + [(0, 0, k) for k in range(1, depth)]
    bit = 1
    while bit < planes:
        peers.append((0, bit, 0))
        bit *= 2
    barrier = pltpu.get_barrier_semaphore()
    for peer in peers:
        pl.semaphore_signal(barrier, inc=1, device_id=device(*peer), device_id_type=MESH)
    pl.semaphore_wait(barrier, len(peers))

    piece = rows // CHUNKS

    def remote(layer, src, dst, h, hop):
        place = pl.ds(h * piece, piece)
        sem = slot_id(*dst) * CHUNKS + h
        return pltpu.make_async_remote_copy(
            src_ref=got[layer].at[slot_id(*src), place],
            dst_ref=got[layer].at[slot_id(*dst), place],
            send_sem=send_sems.at[layer, sem],
            recv_sem=recv_sems.at[layer, sem],
            device_id=device(*hop),
            device_id_type=MESH,
        )

    def forwards(layer, d, k, h):
        copies = []
        bit = 1
        while bit < planes:
            wider = d | bit
            if wider != d and hop_bit(wider, k + h) == bit and not by_column(wider, k, h):
                copies.append(remote(layer, (0, d, k), (0, d | bit, k), h, (0, bit, 0)))
            bit *= 2
        if k == 0:
            for far in range(1, depth):
                if d == 0 or by_column(d, far, h):
                    copies.append(remote(layer, (0, d, 0), (0, d, far), h, (0, 0, far)))
        copies.append(remote(layer, (0, d, k), (1, d, k), h, (1, 0, 0)))
        return copies

    def wait_piece(layer, slot, h):
        remote(layer, slot, slot, h, (1, 0, 0)).wait_recv()

    order = arrival_order(planes, depth)
    size = GROUP * CHUNKS
    groups = [order[i:i + size] for i in range(0, len(order), size)]
    done = []
    folds = []
    waiting = []
    for group in groups:
        ready = []
        for d, k, h in group:
            done.append((d, k))
            if done.count((d, k)) == CHUNKS:
                ready.append((d, k))
        folds.append([(1, d, k) for d, k in waiting] + [(0, d, k) for d, k in ready])
        waiting = ready
    folds.append([(1, d, k) for d, k in waiting])
    uses = [(layer, slot) for layer in range(2) for fold in folds for slot in fold]

    def cache_copy(u):
        layer, slot = uses[u]
        start = pl.multiple_of(block_of(slot) * rows, rows)
        return pltpu.make_async_copy(
            caches[layer].at[pl.ds(start, rows)],
            cached.at[u % CACHE_SLOTS],
            cache_sems.at[u % CACHE_SLOTS],
        )

    def fold_slots(layer, fold, first_use):
        slot_values = [jnp.int32(slot_id(*s)) for s in fold]
        block_values = [block_of(s) for s in fold]

        def body(i, carry):
            s = pick(i, slot_values)
            j = pick(i, block_values)
            code = code_ref[layer, j]
            new = got[layer][s]
            old = cached[(first_use + i) % CACHE_SLOTS]
            change = new.astype(jnp.float32) - old.astype(jnp.float32)
            change = change * change
            parts[layer, j] = jnp.sum(change.reshape(rows // 8, 8, width), axis=0)
            source = lax.select(code >= 4, new, old)
            chosen = lax.select((code // 2) % 2 == 0, source[:tile_rows], source[tile_rows:])
            zeros = jnp.zeros_like(chosen)
            upper = code % 2 == 0
            spread = jnp.concatenate(
                [lax.select(upper, chosen, zeros), lax.select(upper, zeros, chosen)], axis=1
            )
            acc[...] += jnp.dot(tiles_v[j], spread, preferred_element_type=jnp.float32)
            return carry

        lax.fori_loop(0, len(fold), body, 0)

    use = 0
    tile_copy = pltpu.make_async_copy(tiles_ref.at[0], tiles_v, tile_sem)
    sent = []
    for layer in range(2):
        weight = (w1_ref, w2_ref)[layer]
        if layer == 0:
            feat_copy.wait()
        for g, fold in enumerate(folds):
            if g < len(groups):
                for d, k, h in groups[g]:
                    if (d, k) != (0, 0):
                        wait_piece(layer, (0, d, k), h)
                    for copy in forwards(layer, d, k, h):
                        copy.start()
                        sent.append(copy)
                    if layer == 0 and (d, k, h) == (0, 0, 0):
                        tile_copy.start()
                        for u in range(min(CACHE_SLOTS, len(uses))):
                            cache_copy(u).start()
                        acc[...] = jnp.zeros_like(acc)
            if layer == 0 and g == 0:
                tile_copy.wait()
            for t, slot in enumerate(fold):
                if slot[0] == 1:
                    for h in range(CHUNKS):
                        wait_piece(layer, slot, h)
                cache_copy(use + t).wait()
            fold_slots(layer, fold, use)
            for t in range(len(fold)):
                if use + t + CACHE_SLOTS < len(uses):
                    cache_copy(use + t + CACHE_SLOTS).start()
            use += len(fold)
        for part in range(2):
            agg = acc[:, part * width:(part + 1) * width].astype(jnp.bfloat16)
            mixed = jnp.dot(agg, weight[...], preferred_element_type=jnp.float32)
            place = pl.ds(part * tile_rows, tile_rows)
            if layer == 0:
                got_b[0, place] = jnp.maximum(mixed, 0.0).astype(jnp.bfloat16)
            else:
                out_ref[place] = mixed.astype(jnp.bfloat16)
        if layer == 0:
            acc[...] = jnp.zeros_like(acc)
    for layer in range(2):
        total = jnp.sum(jnp.sum(parts[layer], axis=0))
        drift_ref[layer] = total / (blocks * rows * width)
    for copy in sent:
        copy.wait_send()


def on_device(planes, depth, features, cache_in, cache_hidden, tiles, tile_pos, order, skip, w_first, w_second):
    own_index = lax.axis_index(("gx", "gy"))
    block_count = order.shape[1]
    rows, width = features.shape
    tile_rows = tiles.shape[2]
    ids = jnp.arange(block_count, dtype=jnp.int32)
    hits = order[:, :, None] == ids[None, None, :]
    fresh = jnp.sum(jnp.where(hits, (1 - skip)[:, :, None], 0), axis=1)
    fresh = jnp.where(ids[None, :] == own_index, 1, fresh)
    code = fresh * 4 + (tile_pos[0, :, 1] * 2 + tile_pos[0, :, 0])[None, :]
    vmem = pl.BlockSpec(memory_space=pltpu.VMEM)
    smem = pl.BlockSpec(memory_space=pltpu.SMEM)
    anywhere = pl.BlockSpec(memory_space=pl.ANY)
    return pl.pallas_call(
        functools.partial(kernel, planes, depth),
        out_shape=(
            jax.ShapeDtypeStruct((rows, width), jnp.bfloat16),
            jax.ShapeDtypeStruct((2,), jnp.float32),
        ),
        in_specs=[smem, anywhere, anywhere, anywhere, anywhere, vmem, vmem],
        out_specs=(vmem, smem),
        scratch_shapes=[
            pltpu.VMEM((block_count, rows, width), jnp.bfloat16),
            pltpu.VMEM((block_count, rows, width), jnp.bfloat16),
            pltpu.VMEM((block_count, tile_rows, tile_rows), jnp.bfloat16),
            pltpu.VMEM((CACHE_SLOTS, rows, width), jnp.bfloat16),
            pltpu.VMEM((tile_rows, 2 * width), jnp.float32),
            pltpu.VMEM((2, block_count, 8, width), jnp.float32),
            pltpu.SemaphoreType.DMA((2, block_count * CHUNKS)),
            pltpu.SemaphoreType.DMA((2, block_count * CHUNKS)),
            pltpu.SemaphoreType.DMA((CACHE_SLOTS,)),
            pltpu.SemaphoreType.DMA,
            pltpu.SemaphoreType.DMA,
        ],
        compiler_params=pltpu.CompilerParams(
            collective_id=0, has_side_effects=True, vmem_limit_bytes=60 * 1024 * 1024
        ),
    )(code, features, cache_in, cache_hidden, tiles, w_first, w_second)


def solution(mesh):
    in_specs = (
        P(("gx", "gy"), None),
        P(),
        P(),
        P(("gx", "gy"), None, None, None),
        P(("gx", "gy"), None, None),
        P(),
        P(),
        P(),
        P(),
    )
    out_specs = (P(("gx", "gy"), None), P())
    body = functools.partial(on_device, mesh.shape["gx"] // 2, mesh.shape["gy"])
    return jax.shard_map(body, mesh=mesh, in_specs=in_specs, out_specs=out_specs, check_vma=False)
```

```python
import functools

import jax
import jax.numpy as jnp
from jax import lax
from jax.experimental import pallas as pl
from jax.experimental.pallas import tpu as pltpu
from jax.sharding import PartitionSpec as P

GROUP = 4
CACHE_SLOTS = 16
CHUNKS = 2
COLUMN_COST = 2
PLANE_COST = 3
CHUNK_COST = 1
COLUMN_SHARE = 2
MESH = pl.DeviceIdType.MESH


def flip(value, bits):
    bit = 1
    while bit <= bits:
        if bits & bit:
            value = value + bit - 2 * bit * ((value // bit) % 2)
        bit *= 2
    return value


def hop_bit(d, part):
    low = d & -d
    high = 1 << (d.bit_length() - 1)
    return low if part % 2 == 0 else high


def by_column(d, k, part):
    return d & (d - 1) != 0 and 0 < k * CHUNKS + part < COLUMN_SHARE + CHUNKS and k > 0


def pick(i, values):
    chosen = values[0]
    for t in range(1, len(values)):
        chosen = jnp.where(i == t, values[t], chosen)
    return chosen


def arrival_order(planes, depth):
    events = [(d, k, h) for d in range(planes) for k in range(depth) for h in range(CHUNKS)]

    def expected(event):
        d, k, h = event
        return (COLUMN_COST * k + PLANE_COST * bin(d).count("1") + CHUNK_COST * h, k, d, h)

    return sorted(events, key=expected)


def kernel(planes, depth, code_ref, feat_ref, cache_a, cache_b, tiles_ref, w1_ref, w2_ref,
           out_ref, drift_ref, got_a, got_b, tiles_v, cached, acc, parts,
           send_sems, recv_sems, cache_sems, tile_sem, feat_sem):
    half = planes * depth
    blocks = 2 * half
    rows = feat_ref.shape[0]
    tile_rows = rows // 2
    width = feat_ref.shape[1]
    gx = lax.axis_index("gx")
    gz = lax.axis_index("gy")
    plane = gx // 2
    core = gx % 2

    def device(c, d, k):
        return (flip(plane, d) * 2 + flip(core, c), flip(gz, k))

    def block_of(slot):
        x, z = device(*slot)
        return x * depth + z

    def slot_id(c, d, k):
        return c * half + d * depth + k

    got = (got_a, got_b)
    caches = (cache_a, cache_b)

    feat_copy = pltpu.make_async_copy(feat_ref, got_a.at[0], feat_sem)
    feat_copy.start()

    peers = [(1, 0, 0)] + [(0, 0, k) for k in range(1, depth)]
    bit = 1
    while bit < planes:
        peers.append((0, bit, 0))
        bit *= 2
    barrier = pltpu.get_barrier_semaphore()
    for peer in peers:
        pl.semaphore_signal(barrier, inc=1, device_id=device(*peer), device_id_type=MESH)
    pl.semaphore_wait(barrier, len(peers))

    piece = rows // CHUNKS

    def remote(layer, src, dst, h, hop):
        place = pl.ds(h * piece, piece)
        sem = slot_id(*dst) * CHUNKS + h
        return pltpu.make_async_remote_copy(
            src_ref=got[layer].at[slot_id(*src), place],
            dst_ref=got[layer].at[slot_id(*dst), place],
            send_sem=send_sems.at[layer, sem],
            recv_sem=recv_sems.at[layer, sem],
            device_id=device(*hop),
            device_id_type=MESH,
        )

    def forwards(layer, d, k, h):
        copies = []
        bit = 1
        while bit < planes:
            wider = d | bit
            if wider != d and hop_bit(wider, k + h) == bit and not by_column(wider, k, h):
                copies.append(remote(layer, (0, d, k), (0, d | bit, k), h, (0, bit, 0)))
            bit *= 2
        if k == 0:
            for far in range(1, depth):
                if d == 0 or by_column(d, far, h):
                    copies.append(remote(layer, (0, d, 0), (0, d, far), h, (0, 0, far)))
        copies.append(remote(layer, (0, d, k), (1, d, k), h, (1, 0, 0)))
        return copies

    def wait_piece(layer, slot, h):
        remote(layer, slot, slot, h, (1, 0, 0)).wait_recv()

    order = arrival_order(planes, depth)
    size = GROUP * CHUNKS
    groups = [order[i:i + size] for i in range(0, len(order), size)]
    done = []
    folds = []
    waiting = []
    for group in groups:
        ready = []
        for d, k, h in group:
            done.append((d, k))
            if done.count((d, k)) == CHUNKS:
                ready.append((d, k))
        folds.append([(1, d, k) for d, k in waiting] + [(0, d, k) for d, k in ready])
        waiting = ready
    folds.append([(1, d, k) for d, k in waiting])
    uses = [(layer, slot) for layer in range(2) for fold in folds for slot in fold]

    def cache_copy(u):
        layer, slot = uses[u]
        start = pl.multiple_of(block_of(slot) * rows, rows)
        return pltpu.make_async_copy(
            caches[layer].at[pl.ds(start, rows)],
            cached.at[u % CACHE_SLOTS],
            cache_sems.at[u % CACHE_SLOTS],
        )

    def fold_slots(layer, fold, first_use):
        slot_values = [jnp.int32(slot_id(*s)) for s in fold]
        block_values = [block_of(s) for s in fold]

        def body(i, carry):
            s = pick(i, slot_values)
            j = pick(i, block_values)
            code = code_ref[layer, j]
            new = got[layer][s]
            old = cached[(first_use + i) % CACHE_SLOTS]
            change = new.astype(jnp.float32) - old.astype(jnp.float32)
            change = change * change
            parts[layer, j] = jnp.sum(change.reshape(rows // 8, 8, width), axis=0)
            source = lax.select(code >= 4, new, old)
            chosen = lax.select((code // 2) % 2 == 0, source[:tile_rows], source[tile_rows:])
            zeros = jnp.zeros_like(chosen)
            upper = code % 2 == 0
            spread = jnp.concatenate(
                [lax.select(upper, chosen, zeros), lax.select(upper, zeros, chosen)], axis=1
            )
            acc[...] += jnp.dot(tiles_v[j], spread, preferred_element_type=jnp.float32)
            return carry

        lax.fori_loop(0, len(fold), body, 0)

    use = 0
    tile_copy = pltpu.make_async_copy(tiles_ref.at[0], tiles_v, tile_sem)
    sent = []
    for layer in range(2):
        weight = (w1_ref, w2_ref)[layer]
        if layer == 0:
            feat_copy.wait()
        for g, fold in enumerate(folds):
            if g < len(groups):
                for d, k, h in groups[g]:
                    if (d, k) != (0, 0):
                        wait_piece(layer, (0, d, k), h)
                    for copy in forwards(layer, d, k, h):
                        copy.start()
                        sent.append(copy)
                    if layer == 0 and (d, k, h) == (0, 0, 0):
                        tile_copy.start()
                        for u in range(min(CACHE_SLOTS, len(uses))):
                            cache_copy(u).start()
                        acc[...] = jnp.zeros_like(acc)
            if layer == 0 and g == 0:
                tile_copy.wait()
            for t, slot in enumerate(fold):
                if slot[0] == 1:
                    for h in range(CHUNKS):
                        wait_piece(layer, slot, h)
                cache_copy(use + t).wait()
            fold_slots(layer, fold, use)
            for t in range(len(fold)):
                if use + t + CACHE_SLOTS < len(uses):
                    cache_copy(use + t + CACHE_SLOTS).start()
            use += len(fold)
        for part in range(2):
            agg = acc[:, part * width:(part + 1) * width].astype(jnp.bfloat16)
            mixed = jnp.dot(agg, weight[...], preferred_element_type=jnp.float32)
            place = pl.ds(part * tile_rows, tile_rows)
            if layer == 0:
                got_b[0, place] = jnp.maximum(mixed, 0.0).astype(jnp.bfloat16)
            else:
                out_ref[place] = mixed.astype(jnp.bfloat16)
        if layer == 0:
            acc[...] = jnp.zeros_like(acc)
    for layer in range(2):
        total = jnp.sum(jnp.sum(parts[layer], axis=0))
        drift_ref[layer] = total / (blocks * rows * width)
    for copy in sent:
        copy.wait_send()


def on_device(planes, depth, features, cache_in, cache_hidden, tiles, tile_pos, order, skip, w_first, w_second):
    own_index = lax.axis_index(("gx", "gy"))
    block_count = order.shape[1]
    rows, width = features.shape
    tile_rows = tiles.shape[2]
    ids = jnp.arange(block_count, dtype=jnp.int32)
    hits = order[:, :, None] == ids[None, None, :]
    fresh = 1 - jnp.sum(jnp.where(hits, skip[:, :, None], 0), axis=1)
    fresh = jnp.where(ids[None, :] == own_index, 1, fresh)
    code = fresh * 4 + (tile_pos[0, :, 1] * 2 + tile_pos[0, :, 0])[None, :]
    vmem = pl.BlockSpec(memory_space=pltpu.VMEM)
    smem = pl.BlockSpec(memory_space=pltpu.SMEM)
    anywhere = pl.BlockSpec(memory_space=pl.ANY)
    return pl.pallas_call(
        functools.partial(kernel, planes, depth),
        out_shape=(
            jax.ShapeDtypeStruct((rows, width), jnp.bfloat16),
            jax.ShapeDtypeStruct((2,), jnp.float32),
        ),
        in_specs=[smem, anywhere, anywhere, anywhere, anywhere, vmem, vmem],
        out_specs=(vmem, smem),
        scratch_shapes=[
            pltpu.VMEM((block_count, rows, width), jnp.bfloat16),
            pltpu.VMEM((block_count, rows, width), jnp.bfloat16),
            pltpu.VMEM((block_count, tile_rows, tile_rows), jnp.bfloat16),
            pltpu.VMEM((CACHE_SLOTS, rows, width), jnp.bfloat16),
            pltpu.VMEM((tile_rows, 2 * width), jnp.float32),
            pltpu.VMEM((2, block_count, 8, width), jnp.float32),
            pltpu.SemaphoreType.DMA((2, block_count * CHUNKS)),
            pltpu.SemaphoreType.DMA((2, block_count * CHUNKS)),
            pltpu.SemaphoreType.DMA((CACHE_SLOTS,)),
            pltpu.SemaphoreType.DMA,
            pltpu.SemaphoreType.DMA,
        ],
        compiler_params=pltpu.CompilerParams(
            collective_id=0, has_side_effects=True, vmem_limit_bytes=60 * 1024 * 1024
        ),
    )(code, features, cache_in, cache_hidden, tiles, w_first, w_second)


def solution(mesh):
    in_specs = (
        P(("gx", "gy"), None),
        P(),
        P(),
        P(("gx", "gy"), None, None, None),
        P(("gx", "gy"), None, None),
        P(),
        P(),
        P(),
        P(),
    )
    out_specs = (P(("gx", "gy"), None), P())
    body = functools.partial(on_device, mesh.shape["gx"] // 2, mesh.shape["gy"])
    return jax.shard_map(body, mesh=mesh, in_specs=in_specs, out_specs=out_specs, check_vma=False)
```
